32 devices in a mesh: dp: 4 (over z), vocab: 8 (over y, x, core).
Axes of the slice: x: 2, y: 2, z: 4, core: 2. Of those that a mesh axis runs over, the one named last changes fastest.
Arguments:
- teacher_logits: bfloat16 [1536, 151552], P('dp', 'vocab'), may hold values from -40 to 320, as said below
- student_logits: bfloat16 [1536, 126976], P('dp', 'vocab'), may hold values from -40 to 320, as said below
- tile_dest: int32 [1184, 2], replicated, may hold values from 0 to 991, as said below
- tile_weight: bfloat16 [1184, 2, 128, 128], P('vocab'), may hold values from 0.0009994507 to 1
- token_mask: int32 [1536], P('dp'), may hold values from 0 to 1, as said below
Outputs:
- token_loss: float32 [1536], P('dp')
- mean_loss: float32 [], replicated
The draws below stay inside these ranges and needn't reach their ends.
Inputs may be any that keep to these rules, and one draw needn't show every extreme that they name: `teacher_logits`: Real-valued logits. `student_logits`: Real-valued logits. `tile_dest`: row b names the student blocks of the 2 tiles of teacher block b. Student block s belongs to vocab index s // 124, teacher block b to vocab index b // 148. Of the tiles of the teacher blocks of one vocab index, at most 37 name student blocks of any one vocab index, and exactly 37 do for some vocab index. `token_mask`: at least one token has a 1.
All inputs are finite; a program needn't handle non-finite values.
Results may differ from the reference program's by a relative error of at most 0.0031.
Values may be sent and summed in bfloat16 or wider, within the bound.
A program may use at most 192 MiB of HBM per device.

```python
import math
import jax
import jax.numpy as jnp
from jax import lax

BLOCK = 128
VT = 151552
VS = 126976
K = 2
TOKENS = 1536
TBLOCKS = 1184
SBLOCKS = 992
TB_DEV = 148
SB_DEV = 124
CAP = 37
N_VOCAB = 8


def logit_field(key, row_count, col_count):
    key_base = jax.random.fold_in(key, 0)
    base_vals = jnp.clip(3.0 * jax.random.normal(key_base, (row_count, col_count), jnp.float32), -12.0, 12.0)
    return base_vals


def draw_teacher_logits(key, part):
    return logit_field(jax.random.fold_in(key, 11), TOKENS, VT).astype(jnp.bfloat16)


def draw_student_logits(key, part):
    return logit_field(jax.random.fold_in(key, 17), TOKENS, VS).astype(jnp.bfloat16)


def draw_tile_dest(key, part):
    tile_count = TB_DEV * K
    slot_count = N_VOCAB * CAP

    def one_source(source):
        sub_key = jax.random.fold_in(jax.random.fold_in(key, 29), source)
        key_score, key_pick, key_local = jax.random.split(sub_key, 3)
        position = jnp.arange(slot_count, dtype=jnp.int32)
        scores = jax.random.randint(key_score, (slot_count,), 0, 2 ** 20) * slot_count + position
        chosen = jax.random.randint(key_pick, (), 0, N_VOCAB)
        scores = jnp.where(position // CAP == chosen, scores - 2 ** 30, scores)
        slot_order = jnp.argsort(scores, stable=True)[:tile_count]
        owners = slot_order // CAP
        local_block = jax.random.randint(key_local, (tile_count,), 0, SB_DEV)
        return (owners * SB_DEV + local_block).astype(jnp.int32)
    sources = jax.vmap(one_source)(jnp.arange(N_VOCAB, dtype=jnp.int32))
    return sources.reshape(TBLOCKS, K)


def draw_token_mask(key, part):
    key_bits, key_keep = jax.random.split(jax.random.fold_in(key, 43))
    mask_vals = (jax.random.randint(key_bits, (TOKENS,), 0, 4) > 0).astype(jnp.int32)
    kept = jax.random.randint(key_keep, (), 0, TOKENS)
    position = jnp.arange(TOKENS, dtype=jnp.int32)
    return jnp.where(position == kept, 1, mask_vals).astype(jnp.int32)


def block_levels(stream_key, extent, pieces, smallest, largest):
    def one(dim, shards_of):
        heights = jax.random.uniform(jax.random.fold_in(jax.random.fold_in(stream_key, 6), dim), (shards_of,), jnp.float32, smallest / len(pieces), largest / len(pieces))
        return jnp.repeat(jnp.exp(heights), extent[dim] // shards_of).reshape((-1,) + (1,) * (len(extent) - dim - 1))

    loudness = one(*pieces[0])
    for cut in pieces[1:]:
        loudness = loudness * one(*cut)
    return loudness


def setup_inputs(seed: int = 0) -> dict:
    streams_of = jax.random.split(jax.random.key(seed), 6)
    return {
        "teacher_logits": draw_teacher_logits(jax.random.fold_in(streams_of[5], 71), 0),
        "student_logits": draw_student_logits(jax.random.fold_in(streams_of[5], 71), 0),
        "tile_dest": draw_tile_dest(jax.random.fold_in(streams_of[5], 71), 0),
        "tile_weight": jnp.clip(jnp.exp(math.log(1.0) - 6.9083047 * jax.random.uniform(streams_of[3], (TBLOCKS, K, BLOCK, BLOCK), jnp.float32) ** block_levels(streams_of[3], (TBLOCKS, K, BLOCK, BLOCK), ((0, 8),), -0.2, 0.2)), 0.0009994507, 1.0).astype(jnp.bfloat16),
        "token_mask": draw_token_mask(jax.random.fold_in(streams_of[5], 71), 0),
    }


SMOOTH = 0.1


def reference(teacher_logits, student_logits, tile_dest, tile_weight, token_mask):
    weights = tile_weight.astype(jnp.float32)
    mapping = (weights / jnp.sum(weights, axis=(1, 3), keepdims=True)).astype(jnp.bfloat16)
    mapping = lax.optimization_barrier(mapping).astype(jnp.float32)
    targets = tile_dest.reshape(-1).astype(jnp.int32)
    row_count = math.gcd(TOKENS, 256)

    def one_block(block_args):
        teacher_vals, student_vals, mask_vals = block_args
        teacher_vals = teacher_vals.astype(jnp.float32)
        maximum = jnp.max(teacher_vals, axis=1, keepdims=True)
        expon = jnp.exp(teacher_vals - maximum)
        teacher_prob = (expon / jnp.sum(expon, axis=1, keepdims=True)).astype(jnp.bfloat16)
        teacher_prob = lax.optimization_barrier(teacher_prob).astype(jnp.float32)
        prob_blocks = teacher_prob.reshape(row_count, TBLOCKS, BLOCK)
        partial_value = jnp.einsum('rbc,bkcd->bkrd', prob_blocks, mapping)
        partial_value = lax.optimization_barrier(partial_value.astype(jnp.bfloat16)).astype(jnp.float32)
        summed = jax.ops.segment_sum(partial_value.reshape(TBLOCKS * K, row_count, BLOCK), targets, num_segments=SBLOCKS)
        mapped = jnp.transpose(summed, (1, 0, 2)).reshape(row_count, VS)
        target = (1.0 - SMOOTH) * mapped + SMOOTH / VS
        student_vals = student_vals.astype(jnp.float32)
        student_max = jnp.max(student_vals, axis=1, keepdims=True)
        student_sum = jnp.sum(jnp.exp(student_vals - student_max), axis=1, keepdims=True)
        student_logp = student_vals - student_max - jnp.log(student_sum)
        token_kl = jnp.sum(target * (jnp.log(target) - student_logp), axis=1)
        return mask_vals.astype(jnp.float32) * token_kl

    token_loss = lax.map(one_block, (teacher_logits.reshape(-1, row_count, VT), student_logits.reshape(-1, row_count, VS), token_mask.reshape(-1, row_count)))
    token_loss = token_loss.reshape(TOKENS)
    counted = jnp.sum(token_mask.astype(jnp.float32))
    mean_loss = jnp.sum(token_loss) / counted
    return token_loss, mean_loss
```

```python
import functools
import math

import jax
import jax.numpy as jnp
from jax import lax
from jax.experimental import pallas as pl
from jax.experimental.pallas import tpu as pltpu
from jax.sharding import PartitionSpec as P

BLOCK = 128
SMOOTH = 0.1
CHUNK = 96
F32 = jnp.float32
BF16 = jnp.bfloat16


def kernel(n, cap, tbd, sbd, chunk, nc, c0, sidx, sblk, rord, rblk, rsrc, keep, last, valid,
           inv_ref, t_hbm, s_hbm, w_hbm, out_ref,
           tbuf, stbuf, wbuf, prob, sbuf, rbuf0, rbuf1, st_send, st_recv, tr, scl, smx, xbuf,
           in_sem, send_sem, recv_sem, sts_sem, str_sem, credit):
    me = lax.axis_index("vocab")
    slots = n * cap
    rbuf = (rbuf0, rbuf1)
    order = list(range(2, n, 2)) + list(range(3, n, 2)) + [1]
    peers = [me ^ j for j in order]
    shape = (chunk, BLOCK)
    zeros = jnp.zeros(shape, F32)
    lane = lax.broadcasted_iota(jnp.int32, shape, 1)

    def cols(b):
        return pl.ds(pl.multiple_of(b * BLOCK, BLOCK), BLOCK)

    def load_t(c):
        return pltpu.make_async_copy(t_hbm.at[pl.ds(c * chunk, chunk)], tbuf, in_sem.at[0])

    def load_s(c):
        return pltpu.make_async_copy(s_hbm.at[pl.ds(c * chunk, chunk)], stbuf, in_sem.at[1])

    load_w = pltpu.make_async_copy(w_hbm, wbuf, in_sem.at[2])
    load_t(0).start()
    load_w.start()

    barrier = pltpu.get_barrier_semaphore()
    for d in peers:
        pl.semaphore_signal(barrier, inc=1, device_id={"vocab": d})
    pl.semaphore_wait(barrier, n - 1)

    tr[...] = jnp.zeros_like(tr)

    def tile_copy(par, d):
        return pltpu.make_async_remote_copy(
            src_ref=sbuf.at[par, d], dst_ref=rbuf[par].at[pl.ds(me * cap, cap)],
            send_sem=send_sem.at[par, d], recv_sem=recv_sem.at[par, me],
            device_id={"vocab": d})

    def tile_wait(par, src):
        return pltpu.make_async_remote_copy(
            src_ref=sbuf.at[par, src], dst_ref=rbuf[par].at[pl.ds(src * cap, cap)],
            send_sem=send_sem.at[par, src], recv_sem=recv_sem.at[par, src],
            device_id={"vocab": src})

    def stat_copy(par, d):
        return pltpu.make_async_remote_copy(
            src_ref=st_send.at[par], dst_ref=st_recv.at[par, me],
            send_sem=sts_sem.at[par, d], recv_sem=str_sem.at[par, me],
            device_id={"vocab": d})

    def stat_wait(par, src):
        return pltpu.make_async_remote_copy(
            src_ref=st_send.at[par], dst_ref=st_recv.at[par, src],
            send_sem=sts_sem.at[par, src], recv_sem=str_sem.at[par, src],
            device_id={"vocab": src})

    def bcast(column):
        return jnp.broadcast_to(column, shape)

    def produce(c):
        par = c % 2
        load_t(c).wait()
        tmax = lax.fori_loop(
            0, tbd, lambda b, m: jnp.maximum(m, tbuf[:, cols(b)].astype(F32)),
            jnp.full(shape, -jnp.inf, F32), unroll=2)
        tmax = bcast(jnp.max(tmax, axis=1, keepdims=True))

        def expo(b, total):
            e = jnp.exp(tbuf[:, cols(b)].astype(F32) - tmax)
            prob[b] = (e * inv_ref[pl.ds(b, 1), :]).astype(BF16)
            return total + e

        total = lax.fori_loop(0, tbd, expo, zeros, unroll=2)
        if c + 1 < nc:
            load_t(c + 1).start()
        tsum = bcast(jnp.sum(total, axis=1, keepdims=True))
        stat = jnp.where(lane == 0, tmax, jnp.where(lane == 1, tsum, 0.0))
        if chunk < BLOCK:
            stat = jnp.concatenate([stat, jnp.zeros((BLOCK - chunk, BLOCK), F32)], axis=0)
        if c >= 2:
            for d in peers:
                stat_copy(par, d).wait_send()
        rows = stat.T[:8]
        st_send[par] = rows
        st_recv[par, me] = rows
        if c == 0:
            load_w.wait()

        def compute(d, dst):
            def one(r, carry):
                i = sidx[d * cap + r]
                b = sblk[d * cap + r]
                dst[r] = jnp.dot(prob[b], wbuf[i], preferred_element_type=F32).astype(BF16)
                return carry
            lax.fori_loop(0, cap, one, 0, unroll=4)

        for d in peers:
            if c >= 2:
                tile_copy(par, d).wait_send()
            compute(d, sbuf.at[par, d])
            if c >= 2:
                pl.semaphore_wait(credit.at[d], 1)
            stat_copy(par, d).start()
            tile_copy(par, d).start()
        compute(me, rbuf[par].at[pl.ds(me * cap, cap)])

    def student(c):
        load_s(c).wait()
        m = lax.fori_loop(
            0, sbd, lambda b, m: jnp.maximum(m, stbuf[:, cols(b)].astype(F32)),
            jnp.full(shape, -jnp.inf, F32), unroll=2)
        m = bcast(jnp.max(m, axis=1, keepdims=True))
        smx[...] = m

        def step(b, carry):
            total, lin = carry
            x = stbuf[:, cols(b)].astype(F32) - m
            xbuf[b] = x
            return total + jnp.exp(x), lin + x

        total, lin = lax.fori_loop(0, sbd, step, (zeros, zeros), unroll=2)
        if c + 1 < nc:
            load_s(c + 1).start()
        return (jnp.sum(total, axis=1, keepdims=True), jnp.sum(lin, axis=1, keepdims=True))

    def consume(c):
        par = c % 2
        ssum, slin = student(c)
        for d in peers:
            stat_wait(par, d).wait_recv()
        groups = (n * 8 + BLOCK - 1) // BLOCK
        per = BLOCK // 8
        columns = []
        for g in range(groups):
            for j in range(min(per, n - g * per)):
                tr[j * 8:j * 8 + 8, :] = st_recv[par, g * per + j]
            block = tr[...].T
            for j in range(min(per, n - g * per)):
                columns.append((block[:chunk, 8 * j:8 * j + 1], block[:chunk, 8 * j + 1:8 * j + 2]))
        gmax = functools.reduce(jnp.maximum, [m for m, _ in columns])
        gsum = sum(s * jnp.exp(m - gmax) for m, s in columns)
        for j, (m, _) in enumerate(columns):
            scl[j] = bcast(jnp.exp(m - gmax) / gsum)
        for d in peers:
            tile_wait(par, d).wait_recv()
        clogc = c0 * math.log(c0)

        def step(i, carry):
            acc, mass, lin, ent = carry
            o = rord[i]
            src = rsrc[i]
            t = rbuf[par][o].astype(F32) * (scl[src] * valid[i])
            x = xbuf[rblk[i]]
            acc = acc * keep[i] + t
            tgt = (1.0 - SMOOTH) * acc + c0
            ent = ent + last[i] * (tgt * jnp.log(tgt) - clogc)
            return acc, mass + t, lin + t * x, ent

        _, mass, lin, ent = lax.fori_loop(0, slots, step, (zeros,) * 4, unroll=2)
        mass, lin, ent = [jnp.sum(v, axis=1, keepdims=True) for v in (mass, lin, ent)]
        count = sbd * BLOCK
        kla = ent + count * clogc - (1.0 - SMOOTH) * lin - c0 * slin
        tot = (1.0 - SMOOTH) * mass + count * c0
        out_ref[pl.ds(c * chunk, chunk), :] = jnp.where(
            lane == 0, kla, jnp.where(lane == 1, tot, jnp.where(lane == 2, smx[...], ssum)))
        if c + 2 < nc:
            for d in peers:
                pl.semaphore_signal(credit.at[me], inc=1, device_id={"vocab": d})

    load_s(0).start()
    for c in range(nc):
        produce(c)
        if c >= 1:
            consume(c - 1)
    consume(nc - 1)
    for c in range(max(nc - 2, 0), nc):
        for d in peers:
            stat_copy(c % 2, d).wait_send()
            tile_copy(c % 2, d).wait_send()


def tables(tile_dest, n, cap, tbd, sbd, me):
    per = tbd * tile_dest.shape[1]
    dest = tile_dest.reshape(n, per)
    owner = dest // sbd
    block = dest % sbd
    i32 = jnp.int32
    before = jnp.arange(per)[:, None] < jnp.arange(per)[None, :]
    mine = lax.dynamic_index_in_dim(owner, me, 0, keepdims=False)
    rank = jnp.sum((mine[:, None] == mine[None, :]) & before, axis=0, dtype=i32)
    slot = mine * cap + rank
    hit = slot[:, None] == jnp.arange(n * cap)[None, :]
    sidx = jnp.sum(jnp.where(hit, jnp.arange(per, dtype=i32)[:, None], 0), axis=0)
    here = owner == me
    rrank = jnp.sum(here[:, :, None] & before[None], axis=1, dtype=i32)
    rhit = here[:, :, None] & (rrank[:, :, None] == jnp.arange(cap))
    rb = jnp.sum(jnp.where(rhit, block[:, :, None] + 1, 0), axis=1).reshape(-1)
    k = n * cap
    ids = jnp.arange(k, dtype=i32)
    key = jnp.where(rb > 0, rb - 1, sbd) * k + ids
    pos = jnp.sum(key[None, :] < key[:, None], axis=1, dtype=i32)
    order = jnp.sum(jnp.where(pos[:, None] == ids[None, :], key[:, None], 0), axis=0)
    blk = order // k
    o = order % k
    valid = (blk < sbd).astype(F32)
    same = blk[1:] == blk[:-1]
    edge = jnp.zeros((1,), bool)
    keep = jnp.concatenate([edge, same]).astype(F32)
    last = (1.0 - jnp.concatenate([same, edge]).astype(F32)) * valid
    return sidx, sidx // tile_dest.shape[1], o, jnp.minimum(blk, sbd - 1), o // cap, keep, last, valid


def local(teacher_logits, student_logits, tile_dest, tile_weight, token_mask):
    n = lax.axis_size("vocab")
    ndp = lax.axis_size("dp")
    me = lax.axis_index("vocab")
    rows = teacher_logits.shape[0]
    tbd = teacher_logits.shape[1] // BLOCK
    sbd = student_logits.shape[1] // BLOCK
    k = tile_dest.shape[1]
    cap = (tbd * k + n - 1) // n
    chunk = math.gcd(rows, CHUNK)
    nc = rows // chunk
    c0 = SMOOTH / (sbd * BLOCK * n)
    tabs = tables(tile_dest, n, cap, tbd, sbd, me)
    inv = 1.0 / jnp.sum(tile_weight.astype(F32), axis=(1, 3))
    weights = tile_weight.reshape(tbd * k, BLOCK, BLOCK)
    smem = pl.BlockSpec(memory_space=pltpu.SMEM)
    anyspec = pl.BlockSpec(memory_space=pl.ANY)
    vmem = pl.BlockSpec(memory_space=pltpu.VMEM)
    dma = pltpu.SemaphoreType.DMA
    out = pl.pallas_call(
        functools.partial(kernel, n, cap, tbd, sbd, chunk, nc, c0),
        out_shape=jax.ShapeDtypeStruct((rows, BLOCK), F32),
        in_specs=[smem] * 8 + [vmem] + [anyspec] * 3,
        out_specs=vmem,
        scratch_shapes=[
            pltpu.VMEM((chunk, tbd * BLOCK), BF16),
            pltpu.VMEM((chunk, sbd * BLOCK), BF16),
            pltpu.VMEM((tbd * k, BLOCK, BLOCK), BF16),
            pltpu.VMEM((tbd, chunk, BLOCK), BF16),
            pltpu.VMEM((2, n, cap, chunk, BLOCK), BF16),
            pltpu.VMEM((n * cap, chunk, BLOCK), BF16),
            pltpu.VMEM((n * cap, chunk, BLOCK), BF16),
            pltpu.VMEM((2, 8, BLOCK), F32),
            pltpu.VMEM((2, n, 8, BLOCK), F32),
            pltpu.VMEM((BLOCK, BLOCK), F32),
            pltpu.VMEM((n, chunk, BLOCK), F32),
            pltpu.VMEM((chunk, BLOCK), F32),
            pltpu.VMEM((sbd, chunk, BLOCK), F32),
            dma((3,)), dma((2, n)), dma((2, n)), dma((2, n)), dma((2, n)),
            pltpu.SemaphoreType.REGULAR((n,)),
        ],
        compiler_params=pltpu.CompilerParams(
            collective_id=0, has_side_effects=True, vmem_limit_bytes=64 * 2**20 - 65536),
    )(*tabs, inv, teacher_logits, student_logits, weights)
    packed = jnp.concatenate([out[:, :4].T, token_mask.astype(F32)[None]], axis=0)
    every = lax.all_gather(packed, ("dp", "vocab")).reshape(ndp, n, 5, rows)
    kla, tot, smax, ssum, mask = [every[:, :, i] for i in range(5)]
    gmax = jnp.max(smax, axis=1)
    lse = gmax + jnp.log(jnp.sum(ssum * jnp.exp(smax - gmax[:, None]), axis=1))
    token_kl = jnp.sum(kla + tot * (lse[:, None] - smax), axis=1)
    mask = mask[:, 0]
    token_loss = mask * token_kl
    mine = lax.dynamic_index_in_dim(token_loss, lax.axis_index("dp"), 0, keepdims=False)
    return mine, jnp.sum(token_loss) / jnp.sum(mask)


def solution(mesh):
    in_specs = (P("dp", "vocab"), P("dp", "vocab"), P(), P("vocab", None, None, None), P("dp"))
    out_specs = (P("dp"), P())
    return jax.shard_map(local, mesh=mesh, in_specs=in_specs, out_specs=out_specs, check_vma=False)
```
